32 devices in a mesh: ens: 1, slab: 32 (over z, y, x, core).
Axes of the slice: x: 2, y: 2, z: 4, core: 2. Of those that a mesh axis runs over, the one named last changes fastest.
Arguments:
- field: bfloat16 [32, 256, 256, 128], P('ens', 'slab'), may hold values from -6 to 6
- w_x: bfloat16 [2, 32, 32, 32], replicated, may hold values from -0.75 to 0.75
- w_y: bfloat16 [2, 32, 32, 32], replicated, may hold values from -0.75 to 0.75
- w_z: bfloat16 [2, 32, 32, 32], replicated, may hold values from -0.75 to 0.75
- w_in: bfloat16 [32, 128], replicated, may hold values from -1 to 1
- b_in: float32 [128], replicated, may hold values from -3 to 3
- w_out: bfloat16 [128, 32], replicated, may hold values from -0.5 to 0.5
- b_out: float32 [32], replicated, may hold values from -2 to 2
Outputs:
- result: bfloat16 [32, 256, 256, 128], P('ens', 'slab')
The draws below stay inside these ranges and needn't reach their ends.
All inputs are finite; a program needn't handle non-finite values.
Results may differ from the reference program's by a relative error of at most 0.0085.
Values may be sent and summed in bfloat16 or wider, within the bound.
A program may use at most 256 MiB of HBM per device.

```python
import math
import jax
import jax.numpy as jnp
from jax import lax

C = 32
M = 32
H = 128
X = 256
Y = 256
Z = 128


def steps_of(key, shape, pieces, least, top_value):
    def one(dim, shards_of):
        steps = jax.random.uniform(jax.random.fold_in(jax.random.fold_in(key, 6), dim), (shards_of,), jnp.float32, least / len(pieces), top_value / len(pieces))
        return jnp.repeat(jnp.exp(steps), shape[dim] // shards_of).reshape((-1,) + (1,) * (len(shape) - dim - 1))

    gain = one(*pieces[0])
    for cut in pieces[1:]:
        gain = gain * one(*cut)
    return gain


def centred(own_key, shape, deviation, limit, pieces=(), kind=jnp.bfloat16):
    entries = jax.random.normal(own_key, shape, jnp.float32) * deviation
    if len(pieces) > 0:
        entries = steps_of(own_key, shape, pieces, -0.22, 0.18) * entries
    return jnp.clip(entries, min=-limit, max=limit).astype(kind)


def setup_inputs(seed: int = 0, part: int = 0) -> dict:
    splits = jax.random.split(jax.random.key(seed), 9)
    own_keys = jax.random.split(jax.random.fold_in(splits[8], part), 9)
    return {
        "field": centred(own_keys[0], (C, X, Y, Z), 1.0, 6.0, ((1, 32),)),
        "w_x": centred(splits[1], (2, M, C, C), (2 * C) ** -0.5, 0.75),
        "w_y": centred(splits[2], (2, M, C, C), (2 * C) ** -0.5, 0.75),
        "w_z": centred(splits[3], (2, M, C, C), (2 * C) ** -0.5, 0.75),
        "w_in": centred(splits[4], (C, H), C ** -0.5, 1.0),
        "b_in": centred(splits[5], (H,), 0.5, 3.0, (), jnp.float32),
        "w_out": centred(splits[6], (H, C), H ** -0.5, 0.5),
        "b_out": centred(splits[7], (C,), 0.3, 2.0, (), jnp.float32),
    }


def tables(length, mode_count):
    position = jnp.arange(length, dtype=jnp.int32)
    frequency = jnp.arange(mode_count, dtype=jnp.int32)
    phase = (position[:, None] * frequency[None, :]) % length
    angles = phase.astype(jnp.float32) * (2.0 * math.pi / length)
    fwd_cos = jnp.cos(angles).astype(jnp.bfloat16)
    fwd_sin = (-jnp.sin(angles)).astype(jnp.bfloat16)
    factor = jnp.where(frequency == 0, 1.0, 2.0).astype(jnp.float32) / length
    inv_cos = (factor[:, None] * jnp.cos(angles).T).astype(jnp.bfloat16)
    inv_sin = (-factor[:, None] * jnp.sin(angles).T).astype(jnp.bfloat16)
    return fwd_cos, fwd_sin, inv_cos, inv_sin


def mix_modes(spec_re, spec_im, weights, pattern):
    w_re = weights[0].astype(jnp.float32)
    w_im = weights[1].astype(jnp.float32)
    real_part = jnp.einsum(pattern, spec_re.astype(jnp.float32), w_re) - jnp.einsum(pattern, spec_im.astype(jnp.float32), w_im)
    imag_part = jnp.einsum(pattern, spec_im.astype(jnp.float32), w_re) + jnp.einsum(pattern, spec_re.astype(jnp.float32), w_im)
    return real_part.astype(jnp.bfloat16), imag_part.astype(jnp.bfloat16)


def one_branch(field, weights, length, forward, mixing, inverse):
    fwd_cos, fwd_sin, inv_cos, inv_sin = tables(length, weights.shape[1])
    values = field.astype(jnp.float32)
    spec_re = jnp.einsum(forward, values, fwd_cos.astype(jnp.float32)).astype(jnp.bfloat16)
    spec_im = jnp.einsum(forward, values, fwd_sin.astype(jnp.float32)).astype(jnp.bfloat16)
    mixed_re, mixed_im = mix_modes(spec_re, spec_im, weights, mixing)
    branch = jnp.einsum(inverse, mixed_re.astype(jnp.float32), inv_cos.astype(jnp.float32))
    branch = branch + jnp.einsum(inverse, mixed_im.astype(jnp.float32), inv_sin.astype(jnp.float32))
    return branch.astype(jnp.bfloat16)


def reference(field, w_x, w_y, w_z, w_in, b_in, w_out, b_out):
    total = one_branch(field, w_x, X, "cxyz,xm->cmyz", "cmyz,mcd->dmyz", "dmyz,mx->dxyz").astype(jnp.float32)
    total = total + one_branch(field, w_y, Y, "cxyz,ym->cxmz", "cxmz,mcd->dxmz", "dxmz,my->dxyz").astype(jnp.float32)
    total = total + one_branch(field, w_z, Z, "cxyz,zm->cmxy", "cmxy,mcd->dmxy", "dmxy,mz->dxyz").astype(jnp.float32)
    summed = total.astype(jnp.bfloat16)
    summed_t = jnp.moveaxis(summed, 1, 0)
    field_t = jnp.moveaxis(field, 1, 0)
    w_in_f = w_in.astype(jnp.float32)
    w_out_f = w_out.astype(jnp.float32)

    def plane(pair):
        summed_p, field_p = pair
        pre_act = jnp.einsum("cyz,ch->hyz", summed_p.astype(jnp.float32), w_in_f) + b_in[:, None, None]
        hidden = jax.nn.gelu(pre_act, approximate=True).astype(jnp.bfloat16)
        output = field_p.astype(jnp.float32) + jnp.einsum("hyz,hc->cyz", hidden.astype(jnp.float32), w_out_f) + b_out[:, None, None]
        return output.astype(jnp.bfloat16)

    result_t = lax.map(plane, (summed_t, field_t))
    return jnp.moveaxis(result_t, 0, 1)
```

```python
import math

import jax
import jax.numpy as jnp
import numpy as np
from jax import lax
from jax.experimental.layout import Layout, with_layout_constraint
from jax.sharding import PartitionSpec as P

CHUNKS = 4


def tables(length, mode_count):
    phase = (np.arange(length)[:, None] * np.arange(mode_count)[None, :]) % length
    angles = phase.astype(np.float32) * np.float32(2.0 * math.pi / length)
    cos, sin = np.cos(angles), np.sin(angles)
    factor = (np.where(np.arange(mode_count) == 0, 1.0, 2.0) / length).astype(np.float32)
    fwd = np.stack([cos, -sin], axis=1)
    inv = np.stack([factor[:, None] * cos.T, -factor[:, None] * sin.T], axis=0)
    return jnp.asarray(fwd, jnp.bfloat16), jnp.asarray(inv, jnp.bfloat16)


def joint_weights(weights):
    re, im = weights[0], weights[1]
    from_re = jnp.stack([re, im], axis=2)
    from_im = jnp.stack([-im, re], axis=2)
    return jnp.stack([from_re, from_im], axis=1)


def mixed_modes(field, weights, fwd, forward, mixing):
    f32 = jnp.float32
    spec = jnp.einsum(forward, field, fwd, preferred_element_type=f32).astype(jnp.bfloat16)
    return jnp.einsum(mixing, spec, weights, preferred_element_type=f32).astype(jnp.bfloat16)


def inverse_of(mixed, inv, inverse):
    branch = jnp.einsum(inverse, mixed, inv, preferred_element_type=jnp.float32)
    return branch.astype(jnp.bfloat16)


def per_device(field, w_x, w_y, w_z, w_in, b_in, w_out, b_out):
    group_size = lax.axis_size("slab")
    len_x = field.shape[1] * group_size
    len_y = field.shape[2]
    len_z = field.shape[3]
    mode_count = w_x.shape[1]
    fwd_x, inv_x = tables(len_x, mode_count)
    fwd_y, inv_y = tables(len_y, mode_count)
    fwd_z, inv_z = tables(len_z, mode_count)
    joint_x, joint_y, joint_z = joint_weights(w_x), joint_weights(w_y), joint_weights(w_z)
    chunks = math.gcd(CHUNKS, len_y // group_size)
    rows = len_y // chunks
    f32 = jnp.float32

    channels, local_x = field.shape[0], field.shape[1]
    owned = rows // group_size
    fwd_x = fwd_x.reshape(group_size, local_x, 2, mode_count)
    inv_x = inv_x.reshape(2, mode_count, group_size, local_x)
    pieces = []
    branches_x = []
    for k in range(chunks):
        piece = lax.slice_in_dim(field, k * rows, (k + 1) * rows, axis=2)
        pieces.append(piece)
        sent = piece.reshape(channels, local_x, group_size, owned, len_z).transpose(2, 3, 0, 1, 4)
        sent = with_layout_constraint(sent, Layout((0, 3, 1, 2, 4)))
        line = lax.all_to_all(sent, "slab", split_axis=0, concat_axis=0, tiled=True)
        mixed = mixed_modes(line, joint_x, fwd_x, "nycxz,nxqm->qcmyz", "qcmyz,mqcpd->pdmyz")
        back = inverse_of(mixed, inv_x, "pdmyz,pmnx->nydxz")
        back = lax.all_to_all(back, "slab", split_axis=0, concat_axis=0, tiled=True)
        branches_x.append(back.transpose(2, 3, 0, 1, 4).reshape(piece.shape))

    mixed_y = mixed_modes(field, joint_y, fwd_y, "cxyz,yqm->qcxmz", "qcxmz,mqcpd->pdxmz")
    mixed_z = mixed_modes(field, joint_z, fwd_z, "cxyz,zqm->qcmxy", "qcmxy,mqcpd->pdmxy")
    result = jnp.zeros(field.shape, jnp.bfloat16)
    for k in range(chunks):
        y_part = inv_y[:, :, k * rows : (k + 1) * rows]
        z_part = lax.slice_in_dim(mixed_z, k * rows, (k + 1) * rows, axis=4)
        branch_y = inverse_of(mixed_y, y_part, "pdxmz,pmy->dxyz")
        branch_z = inverse_of(z_part, inv_z, "pdmxy,pmz->dxyz")
        summed = (
            branches_x[k].astype(f32) + branch_y.astype(f32) + branch_z.astype(f32)
        ).astype(jnp.bfloat16)
        pre_act = (
            jnp.einsum("cxyz,ch->hxyz", summed, w_in, preferred_element_type=f32)
            + b_in[:, None, None, None]
        )
        hidden = jax.nn.gelu(pre_act, approximate=True).astype(jnp.bfloat16)
        output = (
            pieces[k].astype(f32)
            + jnp.einsum("hxyz,hc->cxyz", hidden, w_out, preferred_element_type=f32)
            + b_out[:, None, None, None]
        )
        output = with_layout_constraint(output.astype(jnp.bfloat16), Layout((0, 1, 2, 3)))
        result = lax.dynamic_update_slice_in_dim(result, output, k * rows, axis=2)
    return result


def solution(mesh):
    return jax.shard_map(
        per_device,
        mesh=mesh,
        in_specs=(P("ens", "slab", None, None), P(), P(), P(), P(), P(), P(), P()),
        out_specs=P("ens", "slab", None, None),
        check_vma=False,
    )
```
